32 devices in a mesh: groups: 2 (over x), rows: 16 (over z, y, core).
Axes of the slice: x: 2, y: 2, z: 4, core: 2. Of those that a mesh axis runs over, the one named last changes fastest.
Arguments:
- phase: float32 [512, 2048], P(('groups', 'rows')), parts along dimension 0, may hold values from -3.140625 to 3.140625
Outputs:
- filtered: float32 [2, 512, 2048], P(None, ('groups', 'rows')), parts along dimension 1
- profile: float32 [6, 16], P('groups'), parts along dimension 0
The draws below stay inside these ranges and needn't reach their ends.
There are 2 independent parts, one for each index of `groups`. The reference program is written for one: setup_inputs(seed, part) draws one part's arguments, and reference() takes and returns one part's arrays. A program takes and returns all parts, laid end to end along the dimension named above; each array names one. Nothing has to cross between parts.
All inputs are finite; a program needn't handle non-finite values.
Results may differ from the reference program's by a relative error of at most 0.00012.
Values sent between devices are 32-bit elements; how exact they have to be, the bound alone decides.
A program may use at most 64 MiB of HBM per device.

```python
import jax
import jax.numpy as jnp
from jax import lax

COLS = 2048
ITERS = 3
NR = 256


def setup_inputs(seed: int = 0, part: int = 0) -> dict:
    streams_of = jax.random.split(jax.random.key(seed), 2)
    part_splits = jax.random.split(jax.random.fold_in(streams_of[1], part), 2)
    phase = jnp.clip(jax.random.uniform(part_splits[0], (NR, COLS), jnp.float32, -3.140625, 3.140625), -3.140625, 3.140625)
    return {"phase": phase}


EPS = 1e-6


def residue_sums(padded_rows):
    padded = jnp.pad(padded_rows, ((0, 0), (0, 0), (0, 1)))
    first = padded[:, :-1, :-1]
    second = padded[:, :-1, 1:]
    third = padded[:, 1:, 1:]
    fourth = padded[:, 1:, :-1]

    def cross(left, right):
        return left[1] * right[0] - left[0] * right[1]

    loop = cross(first, second) + cross(second, third) + cross(third, fourth) + cross(fourth, first)
    height = loop.shape[0]
    return jnp.sum((loop * loop).reshape(height, COLS // 128, 128), axis=(0, 2))


def goldstein(field, taper):
    extended = jnp.pad(field, ((0, 0), (0, 16), (0, 16)))
    blocks = extended.reshape(2, NR // 16 + 1, 16, COLS // 16 + 1, 16)

    def one_row(start):
        strip = lax.dynamic_slice_in_dim(blocks, start, 2, 1).reshape(2, 32, COLS // 16 + 1, 16)
        windows = jnp.concatenate([strip[:, :, :-1], strip[:, :, 1:]], axis=3)
        signal = windows[0] + 1j * windows[1]
        spectrum = jnp.fft.fft2(signal, axes=(0, 2))
        power = spectrum.real ** 2 + spectrum.imag ** 2
        average = jnp.mean(power, axis=(0, 2), keepdims=True)
        result = jnp.fft.ifft2(spectrum * (power / (average + EPS)) ** 0.25, axes=(0, 2)) * taper
        return jnp.stack([result.real, result.imag])

    pieces = lax.map(one_row, jnp.arange(NR // 16, dtype=jnp.int32))
    righty = jnp.pad(pieces[..., 16:], ((0, 0), (0, 0), (0, 0), (1, 0), (0, 0)))[:, :, :, :-1]
    columns = (pieces[..., :16] + righty).reshape(NR // 16, 2, 32, COLS)
    lower = jnp.pad(columns[:, :, 16:], ((1, 0), (0, 0), (0, 0), (0, 0)))[:-1]
    joined = columns[:, :, :16] + lower
    return joined.transpose(1, 0, 2, 3).reshape(2, NR, COLS)


def reference(phase):
    field = jnp.stack([jnp.cos(phase), jnp.sin(phase)])
    offsets = jnp.arange(32, dtype=jnp.float32)
    ramp = 1.0 - jnp.abs(offsets - 15.5) / 16.0
    taper = ramp[:, None, None] * ramp[None, None, :]
    reports = []
    for step in range(ITERS):
        padded_rows = jnp.pad(field, ((0, 0), (0, 1), (0, 0)))
        reports.append(residue_sums(padded_rows) / (NR * 128.0))
        field = goldstein(field, taper)
    return field, jnp.stack(reports)
```

```python
import functools
import math

import jax
import jax.numpy as jnp
from jax import lax
from jax.experimental import pallas as pl
from jax.experimental.pallas import tpu as pltpu
from jax.sharding import PartitionSpec as P

ITERS = 3
HALF = 16
WIN = 32
EPS = 1e-06
REACH = ITERS
SLABS = 2 * REACH + 1


def rotated(value, cosine, sine):
    real, imag = value
    if sine == 0.0:
        return value
    if cosine == 0.0:
        return (imag, -real) if sine > 0 else (-imag, real)
    if abs(cosine - sine) < 1e-12:
        return ((real + imag) * cosine, (imag - real) * cosine)
    if abs(cosine + sine) < 1e-12:
        return ((real - imag) * cosine, (imag + real) * cosine)
    return (real * cosine + imag * sine, imag * cosine - real * sine)


def twiddle(power, size):
    power = power % size
    exact = {0: (1.0, 0.0), size // 4: (0.0, 1.0), size // 2: (-1.0, 0.0), 3 * size // 4: (0.0, -1.0)}
    if power in exact:
        return exact[power]
    angle = 2.0 * math.pi * power / size
    return math.cos(angle), math.sin(angle)


def plus(a, b):
    return (a[0] + b[0], a[1] + b[1])


def minus(a, b):
    return (a[0] - b[0], a[1] - b[1])


def fft(values):
    size = len(values)
    if size == 1:
        return values
    if size == 2:
        return [plus(values[0], values[1]), minus(values[0], values[1])]
    even = fft(values[0::2])
    first = fft(values[1::4])
    third = fft(values[3::4])
    quarter = size // 4
    result = [None] * size
    for k in range(quarter):
        p = rotated(first[k], *twiddle(k, size))
        q = rotated(third[k], *twiddle(3 * k, size))
        total = plus(p, q)
        gap = minus(p, q)
        result[k] = plus(even[k], total)
        result[k + 2 * quarter] = minus(even[k], total)
        base = even[k + quarter]
        result[k + quarter] = (base[0] + gap[1], base[1] - gap[0])
        result[k + 3 * quarter] = (base[0] - gap[1], base[1] + gap[0])
    return result


def inverse_fft(values):
    swapped = fft([(imag, real) for real, imag in values])
    return [(real, imag) for imag, real in swapped]


def ramp(offset):
    return 1.0 - abs(offset - (WIN - 1) / 2) / HALF


SIN = [(-1.0) ** k / math.factorial(2 * k + 1) for k in range(7)]
COS = [(-1.0) ** k / math.factorial(2 * k) for k in range(8)]


def polynomial(coefficients, x):
    total = coefficients[-1]
    for c in coefficients[-2::-1]:
        total = total * x + c
    return total


def cos_sin(x):
    u = x * 0.5
    u2 = u * u
    s = u * polynomial(SIN, u2)
    c = polynomial(COS, u2)
    return 1.0 - 2.0 * s * s, 2.0 * s * c


def kernel(n, lanes, ph_ref, out_ref, prof_ref, ph, z, spec, cols, mine, heard,
           send_sem, recv_sem, tell_sem, hear_sem):
    me = lax.axis_index("rows")

    def inside(index):
        return jnp.logical_and(index >= 0, index < n)

    barrier = pltpu.get_barrier_semaphore()

    @pl.loop(1, n)
    def _(d):
        other = lax.rem(me + d, n)
        pl.semaphore_signal(barrier, inc=1, device_id={"rows": other}, device_id_type=pl.DeviceIdType.MESH)

    lane = lax.broadcasted_iota(jnp.int32, (8, lanes), 1)

    def next_block(x):
        return jnp.where(lane == lanes - 1, 0.0, pltpu.roll(x, lanes - 1, 1))

    def last_block(x):
        return jnp.where(lane == 0, 0.0, pltpu.roll(x, 1, 1))

    def enter(source, slot):
        @pl.loop(0, HALF)
        def _(t):
            for h in range(2):
                x = source[pl.ds(t * HALF + 8 * h, 8), :]
                c, s = cos_sin(x)
                z[0, slot, 0, pl.ds(t * HALF + 8 * h, 8), :] = c
                z[0, slot, 1, pl.ds(t * HALF + 8 * h, 8), :] = s

    def clear(buffer, slot):
        z[buffer, slot] = jnp.zeros((2, HALF * HALF, lanes), jnp.float32)

    enter(ph_ref, REACH)
    for slot in range(1, SLABS - 1):
        clear(1, slot)
    pl.semaphore_wait(barrier, n - 1)

    def copy(d):
        return pltpu.make_async_remote_copy(
            src_ref=ph_ref,
            dst_ref=ph.at[REACH - d],
            send_sem=send_sem.at[REACH - d],
            recv_sem=recv_sem.at[REACH - d],
            device_id={"rows": me + d},
            device_id_type=pl.DeviceIdType.MESH,
        )

    order = [d for k in range(1, REACH + 1) for d in (-k, k)]
    for d in order:
        @pl.when(inside(me + d))
        def _(d=d):
            copy(d).start()

    def arrive(d):
        slot = REACH + d
        valid = inside(me + d)

        @pl.when(valid)
        def _():
            pltpu.make_async_remote_copy(
                src_ref=ph_ref,
                dst_ref=ph.at[slot],
                send_sem=send_sem.at[slot],
                recv_sem=recv_sem.at[slot],
                device_id={"rows": me + d},
                device_id_type=pl.DeviceIdType.MESH,
            ).wait_recv()
            enter(ph.at[slot], slot)

        @pl.when(jnp.logical_not(valid))
        def _():
            clear(0, slot)

    def profile(buffer, step):
        def row(slot, t):
            real = z[buffer, slot, 0, pl.ds(t * HALF, HALF), :]
            imag = z[buffer, slot, 1, pl.ds(t * HALF, HALF), :]

            def after(x):
                first = next_block(x[0:8])[0:1]
                return jnp.concatenate([x[1:], first], axis=0)

            return real, imag, after(real), after(imag)

        def cross(ar, ai, br, bi):
            return ai * br - ar * bi

        def add(upper, lower, total):
            loop = (
                cross(upper[0], upper[1], upper[2], upper[3])
                + cross(upper[2], upper[3], lower[2], lower[3])
                + cross(lower[2], lower[3], lower[0], lower[1])
                + cross(lower[0], lower[1], upper[0], upper[1])
            )
            return total + loop * loop

        total = lax.fori_loop(
            0, HALF - 1,
            lambda t, total: add(row(REACH, t), row(REACH, t + 1), total),
            jnp.zeros((HALF, lanes), jnp.float32),
        )
        total = add(row(REACH, HALF - 1), row(REACH + 1, 0), total)
        mine[pl.ds(step, 1), :] = jnp.sum(total, axis=0, keepdims=True)

    def window_row(buffer, w):
        upper = REACH + w

        energy = jnp.zeros((8, lanes), jnp.float32)
        for h in range(2):
            values = []
            for t in range(WIN):
                at = pl.ds((t % HALF) * HALF + 8 * h, 8)
                values.append((z[buffer, upper + t // HALF, 0, at, :], z[buffer, upper + t // HALF, 1, at, :]))
            for real, imag in values:
                energy = energy + (real * real + imag * imag)
            for k, value in enumerate(fft(values)):
                for c in range(2):
                    spec[c, pl.ds(k * WIN + 8 * h, 8), :] = value[c]
                    spec[c, pl.ds(k * WIN + HALF + 8 * h, 8), :] = next_block(value[c])
        energy = jnp.broadcast_to(jnp.sum(energy, axis=0, keepdims=True), (8, lanes))
        scale = 1.0 / (energy + next_block(energy) + EPS)

        @pl.loop(0, WIN // 8)
        def _(g):
            values = []
            for s in range(WIN):
                at = pl.ds(g * 8 * WIN + s, 8, stride=WIN)
                values.append((spec[0, at, :], spec[1, at, :]))
            shaped = []
            for real, imag in fft(values):
                ratio = jnp.maximum((real * real + imag * imag) * scale, 1e-37)
                gain = lax.rsqrt(lax.rsqrt(ratio))
                shaped.append((real * gain, imag * gain))
            back = inverse_fft(shaped)
            for s in range(HALF):
                near = ramp(s) / (WIN * WIN)
                far = ramp(s + HALF) / (WIN * WIN)
                for c in range(2):
                    joined = back[s][c] * near + last_block(back[s + HALF][c] * far)
                    cols[c, pl.ds(g * 8 * HALF + s, 8, stride=HALF), :] = joined

        for h in range(2):
            values = []
            for k in range(WIN):
                at = pl.ds(k * HALF + 8 * h, 8)
                values.append((cols[0, at, :], cols[1, at, :]))
            for t, value in enumerate(inverse_fft(values)):
                at = pl.ds((t % HALF) * HALF + 8 * h, 8)
                for c in range(2):
                    z[1 - buffer, upper + t // HALF, c, at, :] += value[c] * ramp(t)

        @pl.when(me + w + 1 == n)
        def _():
            clear(1 - buffer, upper + 1)

    mine[...] = jnp.zeros_like(mine)
    arrive(1)
    profile(0, 0)

    @pl.loop(0, 2 * REACH)
    def _(k):
        half = k // 2
        odd = lax.rem(k, 2)

        @pl.when(k > 0)
        def _():
            arrive(jnp.where(odd == 1, -half - 1, half + 1))

        w = jnp.where(odd == 1, -half - 1, half)

        @pl.when(inside(me + w))
        def _():
            window_row(0, w)

    def tell(d):
        other = lax.rem(me + d, n)
        return pltpu.make_async_remote_copy(
            src_ref=mine,
            dst_ref=heard.at[n - d],
            send_sem=tell_sem.at[d],
            recv_sem=hear_sem.at[n - d],
            device_id={"rows": other},
            device_id_type=pl.DeviceIdType.MESH,
        )

    for step in range(1, ITERS):
        buffer = step % 2
        reach = REACH - step
        profile(buffer, step)
        for slot in range(REACH - reach, REACH + reach + 1):
            clear(1 - buffer, slot)

        @pl.loop(-reach, reach)
        def _(w):
            @pl.when(inside(me + w))
            def _():
                window_row(buffer, w)

            if step == ITERS - 1:
                @pl.when(w == -reach)
                def _():
                    @pl.loop(1, n)
                    def _(d):
                        tell(d).start()

    out_ref[...] = z[ITERS % 2, REACH]

    for d in order:
        @pl.when(inside(me + d))
        def _(d=d):
            copy(d).wait_send()

    def listen(d, total):
        tell(d).wait_send()
        pltpu.make_async_remote_copy(
            src_ref=mine,
            dst_ref=heard.at[d],
            send_sem=tell_sem.at[d],
            recv_sem=hear_sem.at[d],
            device_id={"rows": lax.rem(me + d, n)},
            device_id_type=pl.DeviceIdType.MESH,
        ).wait_recv()
        return total + heard[d]

    prof_ref[...] = lax.fori_loop(1, n, listen, mine[...])


def per_device(n, phase):
    slab, width = phase.shape
    assert slab == HALF
    lanes = width // HALF
    turned = phase.reshape(slab, lanes, HALF).transpose(0, 2, 1).reshape(slab * HALF, lanes)
    area = HALF * HALF
    field, sums = pl.pallas_call(
        functools.partial(kernel, n, lanes),
        out_shape=(
            jax.ShapeDtypeStruct((2, area, lanes), jnp.float32),
            jax.ShapeDtypeStruct((8, lanes), jnp.float32),
        ),
        in_specs=[pl.BlockSpec(memory_space=pltpu.VMEM)],
        out_specs=(pl.BlockSpec(memory_space=pltpu.VMEM), pl.BlockSpec(memory_space=pltpu.VMEM)),
        scratch_shapes=[
            pltpu.VMEM((SLABS, area, lanes), jnp.float32),
            pltpu.VMEM((2, SLABS, 2, area, lanes), jnp.float32),
            pltpu.VMEM((2, WIN * WIN, lanes), jnp.float32),
            pltpu.VMEM((2, WIN * HALF, lanes), jnp.float32),
            pltpu.VMEM((8, lanes), jnp.float32),
            pltpu.VMEM((n, 8, lanes), jnp.float32),
            pltpu.SemaphoreType.DMA((SLABS,)),
            pltpu.SemaphoreType.DMA((SLABS,)),
            pltpu.SemaphoreType.DMA((n,)),
            pltpu.SemaphoreType.DMA((n,)),
        ],
        compiler_params=pltpu.CompilerParams(collective_id=0, has_side_effects=True),
    )(turned)
    filtered = field.reshape(2, slab, HALF, lanes).transpose(0, 1, 3, 2).reshape(2, slab, width)
    per_tile = 128 // HALF
    tiles = sums[:ITERS].reshape(ITERS, lanes // per_tile, per_tile).sum(axis=2)
    return filtered, tiles / (slab * n * 128.0)


def solution(mesh):
    return jax.shard_map(
        functools.partial(per_device, mesh.shape["rows"]),
        mesh=mesh,
        in_specs=(P(("groups", "rows"), None),),
        out_specs=(P(None, ("groups", "rows"), None), P("groups", None)),
        check_vma=False,
    )
```

```python
import functools
import math

import jax
import jax.numpy as jnp
from jax import lax
from jax.experimental import pallas as pl
from jax.experimental.pallas import tpu as pltpu
from jax.sharding import PartitionSpec as P

ITERS = 3
HALF = 16
WIN = 32
EPS = 1e-06
REACH = ITERS
SLABS = 2 * REACH + 1
PITCH = HALF + 1


def rotated(value, cosine, sine):
    real, imag = value
    if sine == 0.0:
        return value
    if cosine == 0.0:
        return (imag, -real) if sine > 0 else (-imag, real)
    if abs(cosine - sine) < 1e-12:
        return ((real + imag) * cosine, (imag - real) * cosine)
    if abs(cosine + sine) < 1e-12:
        return ((real - imag) * cosine, (imag + real) * cosine)
    return (real * cosine + imag * sine, imag * cosine - real * sine)


def twiddle(power, size):
    power = power % size
    exact = {0: (1.0, 0.0), size // 4: (0.0, 1.0), size // 2: (-1.0, 0.0), 3 * size // 4: (0.0, -1.0)}
    if power in exact:
        return exact[power]
    angle = 2.0 * math.pi * power / size
    return math.cos(angle), math.sin(angle)


def plus(a, b):
    return (a[0] + b[0], a[1] + b[1])


def minus(a, b):
    return (a[0] - b[0], a[1] - b[1])


def fft(values):
    size = len(values)
    if size == 1:
        return values
    if size == 2:
        return [plus(values[0], values[1]), minus(values[0], values[1])]
    even = fft(values[0::2])
    first = fft(values[1::4])
    third = fft(values[3::4])
    quarter = size // 4
    result = [None] * size
    for k in range(quarter):
        p = rotated(first[k], *twiddle(k, size))
        q = rotated(third[k], *twiddle(3 * k, size))
        total = plus(p, q)
        gap = minus(p, q)
        result[k] = plus(even[k], total)
        result[k + 2 * quarter] = minus(even[k], total)
        base = even[k + quarter]
        result[k + quarter] = (base[0] + gap[1], base[1] - gap[0])
        result[k + 3 * quarter] = (base[0] - gap[1], base[1] + gap[0])
    return result


def inverse_fft(values):
    swapped = fft([(imag, real) for real, imag in values])
    return [(real, imag) for imag, real in swapped]


def ramp(offset):
    return 1.0 - abs(offset - (WIN - 1) / 2) / HALF


SIN = [(-1.0) ** k / math.factorial(2 * k + 1) for k in range(7)]
COS = [(-1.0) ** k / math.factorial(2 * k) for k in range(8)]


def polynomial(coefficients, x):
    total = coefficients[-1]
    for c in coefficients[-2::-1]:
        total = total * x + c
    return total


def cos_sin(x):
    u = x * 0.5
    u2 = u * u
    s = u * polynomial(SIN, u2)
    c = polynomial(COS, u2)
    return 1.0 - 2.0 * s * s, 2.0 * s * c


def kernel(n, lanes, ph_ref, out_ref, prof_ref, ph, z, spec, cols, mine, heard,
           send_sem, recv_sem, tell_sem, hear_sem):
    me = lax.axis_index("rows")

    def inside(index):
        return jnp.logical_and(index >= 0, index < n)

    barrier = pltpu.get_barrier_semaphore()

    @pl.loop(1, n)
    def _(d):
        other = lax.rem(me + d, n)
        pl.semaphore_signal(barrier, inc=1, device_id={"rows": other}, device_id_type=pl.DeviceIdType.MESH)

    lane = lax.broadcasted_iota(jnp.int32, (8, lanes), 1)

    def next_block(x):
        return jnp.where(lane == lanes - 1, 0.0, pltpu.roll(x, lanes - 1, 1))

    def last_block(x):
        return jnp.where(lane == 0, 0.0, pltpu.roll(x, 1, 1))

    def enter(source, slot):
        @pl.loop(0, HALF)
        def _(t):
            for h in range(2):
                x = source[pl.ds(t * HALF + 8 * h, 8), :]
                c, s = cos_sin(x)
                z[0, slot, 0, pl.ds(t * HALF + 8 * h, 8), :] = c
                z[0, slot, 1, pl.ds(t * HALF + 8 * h, 8), :] = s

    def clear(buffer, slot):
        z[buffer, slot] = jnp.zeros((2, HALF * HALF, lanes), jnp.float32)

    enter(ph_ref, REACH)
    for slot in range(1, SLABS - 1):
        clear(1, slot)
    pl.semaphore_wait(barrier, n - 1)

    def copy(d):
        return pltpu.make_async_remote_copy(
            src_ref=ph_ref,
            dst_ref=ph.at[REACH - d],
            send_sem=send_sem.at[REACH - d],
            recv_sem=recv_sem.at[REACH - d],
            device_id={"rows": me + d},
            device_id_type=pl.DeviceIdType.MESH,
        )

    order = [d for k in range(1, REACH + 1) for d in (-k, k)]
    for d in order:
        @pl.when(inside(me + d))
        def _(d=d):
            copy(d).start()

    def arrive(d):
        slot = REACH + d
        valid = inside(me + d)

        @pl.when(valid)
        def _():
            pltpu.make_async_remote_copy(
                src_ref=ph_ref,
                dst_ref=ph.at[slot],
                send_sem=send_sem.at[slot],
                recv_sem=recv_sem.at[slot],
                device_id={"rows": me + d},
                device_id_type=pl.DeviceIdType.MESH,
            ).wait_recv()
            enter(ph.at[slot], slot)

        @pl.when(jnp.logical_not(valid))
        def _():
            clear(0, slot)

    def profile(buffer, step):
        def row(slot, t):
            real = z[buffer, slot, 0, pl.ds(t * HALF, HALF), :]
            imag = z[buffer, slot, 1, pl.ds(t * HALF, HALF), :]

            def after(x):
                first = next_block(x[0:8])[0:1]
                return jnp.concatenate([x[1:], first], axis=0)

            return real, imag, after(real), after(imag)

        def cross(ar, ai, br, bi):
            return ai * br - ar * bi

        def add(upper, lower, total):
            loop = (
                cross(upper[0], upper[1], upper[2], upper[3])
                + cross(upper[2], upper[3], lower[2], lower[3])
                + cross(lower[2], lower[3], lower[0], lower[1])
                + cross(lower[0], lower[1], upper[0], upper[1])
            )
            return total + loop * loop

        total = lax.fori_loop(
            0, HALF - 1,
            lambda t, total: add(row(REACH, t), row(REACH, t + 1), total),
            jnp.zeros((HALF, lanes), jnp.float32),
        )
        total = add(row(REACH, HALF - 1), row(REACH + 1, 0), total)
        mine[pl.ds(step, 1), :] = jnp.sum(total, axis=0, keepdims=True)

    def window_row(buffer, w):
        upper = REACH + w

        energy = jnp.zeros((8, lanes), jnp.float32)
        for h in range(2):
            values = []
            for t in range(WIN):
                at = pl.ds((t % HALF) * HALF + 8 * h, 8)
                values.append((z[buffer, upper + t // HALF, 0, at, :], z[buffer, upper + t // HALF, 1, at, :]))
            for real, imag in values:
                energy = energy + (real * real + imag * imag)
            for k, value in enumerate(fft(values)):
                for c in range(2):
                    spec[c, pl.ds(k * PITCH + 8 * h, 8), :] = value[c]
        energy = jnp.broadcast_to(jnp.sum(energy, axis=0, keepdims=True), (8, lanes))
        scale = 1.0 / (energy + next_block(energy) + EPS)

        @pl.loop(0, WIN // 8)
        def _(g):
            values = []
            for s in range(HALF):
                at = pl.ds(g * 8 * PITCH + s, 8, stride=PITCH)
                values.append((spec[0, at, :], spec[1, at, :]))
            values += [(next_block(real), next_block(imag)) for real, imag in values]
            shaped = []
            for real, imag in fft(values):
                ratio = jnp.maximum((real * real + imag * imag) * scale, 1e-37)
                gain = lax.rsqrt(lax.rsqrt(ratio))
                shaped.append((real * gain, imag * gain))
            back = inverse_fft(shaped)
            for s in range(HALF):
                near = ramp(s) / (WIN * WIN)
                far = ramp(s + HALF) / (WIN * WIN)
                for c in range(2):
                    joined = back[s][c] * near + last_block(back[s + HALF][c] * far)
                    cols[c, pl.ds(g * 8 * PITCH + s, 8, stride=PITCH), :] = joined

        for h in range(2):
            values = []
            for k in range(WIN):
                at = pl.ds(k * PITCH + 8 * h, 8)
                values.append((cols[0, at, :], cols[1, at, :]))
            for t, value in enumerate(inverse_fft(values)):
                at = pl.ds((t % HALF) * HALF + 8 * h, 8)
                for c in range(2):
                    z[1 - buffer, upper + t // HALF, c, at, :] += value[c] * ramp(t)

        @pl.when(me + w + 1 == n)
        def _():
            clear(1 - buffer, upper + 1)

    mine[...] = jnp.zeros_like(mine)
    arrive(1)
    profile(0, 0)

    @pl.loop(0, 2 * REACH)
    def _(k):
        half = k // 2
        odd = lax.rem(k, 2)

        @pl.when(k > 0)
        def _():
            arrive(jnp.where(odd == 1, -half - 1, half + 1))

        w = jnp.where(odd == 1, -half - 1, half)

        @pl.when(inside(me + w))
        def _():
            window_row(0, w)

    def tell(d):
        other = lax.rem(me + d, n)
        return pltpu.make_async_remote_copy(
            src_ref=mine,
            dst_ref=heard.at[n - d],
            send_sem=tell_sem.at[d],
            recv_sem=hear_sem.at[n - d],
            device_id={"rows": other},
            device_id_type=pl.DeviceIdType.MESH,
        )

    for step in range(1, ITERS):
        buffer = step % 2
        reach = REACH - step
        profile(buffer, step)
        for slot in range(REACH - reach, REACH + reach + 1):
            clear(1 - buffer, slot)

        @pl.loop(-reach, reach)
        def _(w):
            @pl.when(inside(me + w))
            def _():
                window_row(buffer, w)

            if step == ITERS - 1:
                @pl.when(w == -reach)
                def _():
                    @pl.loop(1, n)
                    def _(d):
                        tell(d).start()

    out_ref[...] = z[ITERS % 2, REACH]

    for d in order:
        @pl.when(inside(me + d))
        def _(d=d):
            copy(d).wait_send()

    def listen(d, total):
        tell(d).wait_send()
        pltpu.make_async_remote_copy(
            src_ref=mine,
            dst_ref=heard.at[d],
            send_sem=tell_sem.at[d],
            recv_sem=hear_sem.at[d],
            device_id={"rows": lax.rem(me + d, n)},
            device_id_type=pl.DeviceIdType.MESH,
        ).wait_recv()
        return total + heard[d]

    sums = lax.fori_loop(1, n, listen, mine[...])
    tiles = prof_ref.shape[1]
    per_tile = lanes // tiles
    rows = lax.broadcasted_iota(jnp.int32, (lanes, tiles), 0)
    low = lax.broadcasted_iota(jnp.int32, (lanes, tiles), 1) * per_tile
    member = jnp.where(jnp.logical_and(rows >= low, rows < low + per_tile), 1.0, 0.0)
    energy = jnp.dot(sums, member, precision=lax.Precision.HIGHEST, preferred_element_type=jnp.float32)
    prof_ref[...] = energy[:ITERS] / (HALF * n * 128.0)


def per_device(n, phase):
    slab, width = phase.shape
    assert slab == HALF
    lanes = width // HALF
    turned = phase.reshape(slab, lanes, HALF).transpose(0, 2, 1).reshape(slab * HALF, lanes)
    area = HALF * HALF
    field, profile = pl.pallas_call(
        functools.partial(kernel, n, lanes),
        out_shape=(
            jax.ShapeDtypeStruct((2, area, lanes), jnp.float32),
            jax.ShapeDtypeStruct((ITERS, width // 128), jnp.float32),
        ),
        in_specs=[pl.BlockSpec(memory_space=pltpu.VMEM)],
        out_specs=(pl.BlockSpec(memory_space=pltpu.VMEM), pl.BlockSpec(memory_space=pltpu.VMEM)),
        scratch_shapes=[
            pltpu.VMEM((SLABS, area, lanes), jnp.float32),
            pltpu.VMEM((2, SLABS, 2, area, lanes), jnp.float32),
            pltpu.VMEM((2, WIN * PITCH, lanes), jnp.float32),
            pltpu.VMEM((2, WIN * PITCH, lanes), jnp.float32),
            pltpu.VMEM((8, lanes), jnp.float32),
            pltpu.VMEM((n, 8, lanes), jnp.float32),
            pltpu.SemaphoreType.DMA((SLABS,)),
            pltpu.SemaphoreType.DMA((SLABS,)),
            pltpu.SemaphoreType.DMA((n,)),
            pltpu.SemaphoreType.DMA((n,)),
        ],
        compiler_params=pltpu.CompilerParams(collective_id=0, has_side_effects=True),
    )(turned)
    filtered = field.reshape(2, slab, HALF, lanes).transpose(0, 1, 3, 2).reshape(2, slab, width)
    return filtered, profile


def solution(mesh):
    return jax.shard_map(
        functools.partial(per_device, mesh.shape["rows"]),
        mesh=mesh,
        in_specs=(P(("groups", "rows"), None),),
        out_specs=(P(None, ("groups", "rows"), None), P("groups", None)),
        check_vma=False,
    )
```

```python
import functools
import math

import jax
import jax.numpy as jnp
from jax import lax
from jax.experimental import pallas as pl
from jax.experimental.pallas import tpu as pltpu
from jax.sharding import PartitionSpec as P

ITERS = 3
HALF = 16
WIN = 32
EPS = 1e-06
REACH = ITERS
SLABS = 2 * REACH + 1
PITCH = HALF + 1
AREA = HALF * HALF
SKEW = 8


def rotated(value, cosine, sine):
    real, imag = value
    if sine == 0.0:
        return value
    if cosine == 0.0:
        return (imag, -real) if sine > 0 else (-imag, real)
    if abs(cosine - sine) < 1e-12:
        return ((real + imag) * cosine, (imag - real) * cosine)
    if abs(cosine + sine) < 1e-12:
        return ((real - imag) * cosine, (imag + real) * cosine)
    return (real * cosine + imag * sine, imag * cosine - real * sine)


def twiddle(power, size):
    power = power % size
    exact = {0: (1.0, 0.0), size // 4: (0.0, 1.0), size // 2: (-1.0, 0.0), 3 * size // 4: (0.0, -1.0)}
    if power in exact:
        return exact[power]
    angle = 2.0 * math.pi * power / size
    return math.cos(angle), math.sin(angle)


def plus(a, b):
    return (a[0] + b[0], a[1] + b[1])


def minus(a, b):
    return (a[0] - b[0], a[1] - b[1])


def fft(values):
    size = len(values)
    if size == 1:
        return values
    if size == 2:
        return [plus(values[0], values[1]), minus(values[0], values[1])]
    even = fft(values[0::2])
    first = fft(values[1::4])
    third = fft(values[3::4])
    quarter = size // 4
    result = [None] * size
    for k in range(quarter):
        p = rotated(first[k], *twiddle(k, size))
        q = rotated(third[k], *twiddle(3 * k, size))
        total = plus(p, q)
        gap = minus(p, q)
        result[k] = plus(even[k], total)
        result[k + 2 * quarter] = minus(even[k], total)
        base = even[k + quarter]
        result[k + quarter] = (base[0] + gap[1], base[1] - gap[0])
        result[k + 3 * quarter] = (base[0] - gap[1], base[1] + gap[0])
    return result


def inverse_fft(values):
    swapped = fft([(imag, real) for real, imag in values])
    return [(real, imag) for imag, real in swapped]


def ramp(offset):
    return 1.0 - abs(offset - (WIN - 1) / 2) / HALF


SIN = [(-1.0) ** k / math.factorial(2 * k + 1) for k in range(7)]
COS = [(-1.0) ** k / math.factorial(2 * k) for k in range(8)]


def polynomial(coefficients, x):
    total = coefficients[-1]
    for c in coefficients[-2::-1]:
        total = total * x + c
    return total


def cos_sin(x):
    u = x * 0.5
    u2 = u * u
    s = u * polynomial(SIN, u2)
    c = polynomial(COS, u2)
    return 1.0 - 2.0 * s * s, 2.0 * s * c


def kernel(n, lanes, ph_ref, out_ref, prof_ref, ph, z, spec, cols, mine, heard,
           send_sem, recv_sem, tell_sem, hear_sem):
    me = lax.axis_index("rows")

    def inside(index):
        return jnp.logical_and(index >= 0, index < n)

    barrier = pltpu.get_barrier_semaphore()

    @pl.loop(1, n)
    def _(d):
        other = lax.rem(me + d, n)
        pl.semaphore_signal(barrier, inc=1, device_id={"rows": other}, device_id_type=pl.DeviceIdType.MESH)

    lane = lax.broadcasted_iota(jnp.int32, (8, lanes), 1)

    def next_block(x):
        return jnp.where(lane == lanes - 1, 0.0, pltpu.roll(x, lanes - 1, 1))

    def last_block(x):
        return jnp.where(lane == 0, 0.0, pltpu.roll(x, 1, 1))

    def enter(source, slot):
        @pl.loop(0, HALF)
        def _(t):
            for h in range(2):
                x = source[pl.ds(t * HALF + 8 * h, 8), :]
                c, s = cos_sin(x)
                z[0, slot, 0, pl.ds(t * HALF + 8 * h, 8), :] = c
                z[0, slot, 1, pl.ds(t * HALF + 8 * h, 8), :] = s

    def clear(buffer, slot):
        for c in range(2):
            z[buffer, slot, c, 0:AREA] = jnp.zeros((AREA, lanes), jnp.float32)

    enter(ph_ref, REACH)
    for slot in range(1, SLABS - 1):
        clear(1, slot)
    pl.semaphore_wait(barrier, n - 1)

    side = 1 - 2 * lax.rem(me, 2)

    def copy(source, d, target, index):
        slot = REACH + d - target
        return pltpu.make_async_remote_copy(
            src_ref=source,
            dst_ref=ph.at[slot],
            send_sem=send_sem.at[index],
            recv_sem=recv_sem.at[slot],
            device_id={"rows": me + target},
            device_id_type=pl.DeviceIdType.MESH,
        )

    direct = [(side, 0), (2 * side, 1), (-2 * side, 2), (-3 * side, 3)]
    relayed = [(2 * side, 4), (-2 * side, 5)]

    for target, index in direct:
        @pl.when(inside(me + target))
        def _(target=target, index=index):
            copy(ph_ref, 0, target, index).start()

    def landed(d):
        slot = REACH + d
        return pltpu.make_async_remote_copy(
            src_ref=ph_ref,
            dst_ref=ph.at[slot],
            send_sem=send_sem.at[0],
            recv_sem=recv_sem.at[slot],
            device_id={"rows": me + d},
            device_id_type=pl.DeviceIdType.MESH,
        )

    def relay():
        for d, index in relayed:
            @pl.when(inside(me + d))
            def _(d=d, index=index):
                landed(d).wait_recv()
                copy(ph.at[REACH + d], d, side, index).start()

    def arrive(d, waited):
        slot = REACH + d
        valid = inside(me + d)

        @pl.when(valid)
        def _():
            if not waited:
                landed(d).wait_recv()
            enter(ph.at[slot], slot)

        @pl.when(jnp.logical_not(valid))
        def _():
            clear(0, slot)

    def profile(buffer, step):
        def row(slot, t):
            real = z[buffer, slot, 0, pl.ds(t * HALF, HALF), :]
            imag = z[buffer, slot, 1, pl.ds(t * HALF, HALF), :]

            def after(x):
                first = next_block(x[0:8])[0:1]
                return jnp.concatenate([x[1:], first], axis=0)

            return real, imag, after(real), after(imag)

        def cross(ar, ai, br, bi):
            return ai * br - ar * bi

        def add(upper, lower, total):
            loop = (
                cross(upper[0], upper[1], upper[2], upper[3])
                + cross(upper[2], upper[3], lower[2], lower[3])
                + cross(lower[2], lower[3], lower[0], lower[1])
                + cross(lower[0], lower[1], upper[0], upper[1])
            )
            return total + loop * loop

        total = lax.fori_loop(
            0, HALF - 1,
            lambda t, total: add(row(REACH, t), row(REACH, t + 1), total),
            jnp.zeros((HALF, lanes), jnp.float32),
        )
        total = add(row(REACH, HALF - 1), row(REACH + 1, 0), total)
        mine[pl.ds(step, 1), :] = jnp.sum(total, axis=0, keepdims=True)

    def window_row(buffer, w):
        upper = REACH + w

        energy = jnp.zeros((8, lanes), jnp.float32)
        for h in range(2):
            values = []
            for t in range(WIN):
                at = pl.ds((t % HALF) * HALF + 8 * h, 8)
                values.append((z[buffer, upper + t // HALF, 0, at, :], z[buffer, upper + t // HALF, 1, at, :]))
            for real, imag in values:
                energy = energy + (real * real + imag * imag)
            for k, value in enumerate(fft(values)):
                for c in range(2):
                    spec[c, pl.ds(k * PITCH + 8 * h, 8), :] = value[c]
        energy = jnp.broadcast_to(jnp.sum(energy, axis=0, keepdims=True), (8, lanes))
        scale = 1.0 / (energy + next_block(energy) + EPS)

        @pl.loop(0, WIN // 8)
        def _(g):
            values = []
            for s in range(HALF):
                at = pl.ds(g * 8 * PITCH + s, 8, stride=PITCH)
                values.append((spec[0, at, :], spec[1, at, :]))
            values += [(next_block(real), next_block(imag)) for real, imag in values]
            shaped = []
            for real, imag in fft(values):
                ratio = jnp.maximum((real * real + imag * imag) * scale, 1e-37)
                gain = lax.rsqrt(lax.rsqrt(ratio))
                shaped.append((real * gain, imag * gain))
            back = inverse_fft(shaped)
            for s in range(HALF):
                near = ramp(s) / (WIN * WIN)
                far = ramp(s + HALF) / (WIN * WIN)
                for c in range(2):
                    joined = back[s][c] * near + last_block(back[s + HALF][c] * far)
                    cols[c, pl.ds(g * 8 * PITCH + s, 8, stride=PITCH), :] = joined

        for h in range(2):
            values = []
            for k in range(WIN):
                at = pl.ds(k * PITCH + 8 * h, 8)
                values.append((cols[0, at, :], cols[1, at, :]))
            for t, value in enumerate(inverse_fft(values)):
                at = pl.ds((t % HALF) * HALF + 8 * h, 8)
                for c in range(2):
                    z[1 - buffer, upper + t // HALF, c, at, :] += value[c] * ramp(t)

        @pl.when(me + w + 1 == n)
        def _():
            clear(1 - buffer, upper + 1)

    mine[...] = jnp.zeros_like(mine)

    def first_pass(slab, window, waited):
        arrive(slab * side, waited)
        w = window * side + (side - 1) // 2

        @pl.when(inside(me + w))
        def _():
            window_row(0, w)

    first_pass(1, 0, False)
    relay()
    first_pass(2, 1, True)

    @pl.loop(0, 2)
    def _(k):
        w = -1 - k
        slab = (-1 - k) * side

        @pl.when(k == 0)
        def _():
            arrive(slab, False)

        @pl.when(k == 1)
        def _():
            arrive(slab, True)

        below = w * side + (side - 1) // 2

        @pl.when(inside(me + below))
        def _():
            window_row(0, below)

    @pl.loop(0, 2)
    def _(k):
        slab = (3 - 6 * k) * side
        arrive(slab, False)
        below = (2 - 5 * k) * side + (side - 1) // 2

        @pl.when(inside(me + below))
        def _():
            window_row(0, below)

    profile(0, 0)

    def tell(d):
        other = lax.rem(me + d, n)
        return pltpu.make_async_remote_copy(
            src_ref=mine,
            dst_ref=heard.at[n - d],
            send_sem=tell_sem.at[d],
            recv_sem=hear_sem.at[n - d],
            device_id={"rows": other},
            device_id_type=pl.DeviceIdType.MESH,
        )

    for step in range(1, ITERS):
        buffer = step % 2
        reach = REACH - step
        profile(buffer, step)
        for slot in range(REACH - reach, REACH + reach + 1):
            clear(1 - buffer, slot)

        @pl.loop(-reach, reach)
        def _(w):
            @pl.when(inside(me + w))
            def _():
                window_row(buffer, w)

            if step == ITERS - 1:
                @pl.when(w == -reach)
                def _():
                    @pl.loop(1, n)
                    def _(d):
                        tell(d).start()

    for c in range(2):
        out_ref[c] = z[ITERS % 2, REACH, c, 0:AREA]

    for target, index in direct:
        @pl.when(inside(me + target))
        def _(target=target, index=index):
            copy(ph_ref, 0, target, index).wait_send()

    for d, index in relayed:
        @pl.when(inside(me + d))
        def _(d=d, index=index):
            copy(ph.at[REACH + d], d, side, index).wait_send()

    def listen(d, total):
        tell(d).wait_send()
        pltpu.make_async_remote_copy(
            src_ref=mine,
            dst_ref=heard.at[d],
            send_sem=tell_sem.at[d],
            recv_sem=hear_sem.at[d],
            device_id={"rows": lax.rem(me + d, n)},
            device_id_type=pl.DeviceIdType.MESH,
        ).wait_recv()
        return total + heard[d]

    sums = lax.fori_loop(1, n, listen, mine[...])
    tiles = prof_ref.shape[1]
    per_tile = lanes // tiles
    rows = lax.broadcasted_iota(jnp.int32, (lanes, tiles), 0)
    low = lax.broadcasted_iota(jnp.int32, (lanes, tiles), 1) * per_tile
    member = jnp.where(jnp.logical_and(rows >= low, rows < low + per_tile), 1.0, 0.0)
    energy = jnp.dot(sums, member, precision=lax.Precision.HIGHEST, preferred_element_type=jnp.float32)
    prof_ref[...] = energy[:ITERS] / (HALF * n * 128.0)


def per_device(n, phase):
    slab, width = phase.shape
    assert slab == HALF and n % 2 == 0
    lanes = width // HALF
    turned = phase.reshape(slab, lanes, HALF).transpose(0, 2, 1).reshape(slab * HALF, lanes)
    field, profile = pl.pallas_call(
        functools.partial(kernel, n, lanes),
        out_shape=(
            jax.ShapeDtypeStruct((2, AREA, lanes), jnp.float32),
            jax.ShapeDtypeStruct((ITERS, width // 128), jnp.float32),
        ),
        in_specs=[pl.BlockSpec(memory_space=pltpu.VMEM)],
        out_specs=(pl.BlockSpec(memory_space=pltpu.VMEM), pl.BlockSpec(memory_space=pltpu.VMEM)),
        scratch_shapes=[
            pltpu.VMEM((SLABS, AREA, lanes), jnp.float32),
            pltpu.VMEM((2, SLABS, 2, AREA + SKEW, lanes), jnp.float32),
            pltpu.VMEM((2, WIN * PITCH + SKEW, lanes), jnp.float32),
            pltpu.VMEM((2, WIN * PITCH + SKEW, lanes), jnp.float32),
            pltpu.VMEM((8, lanes), jnp.float32),
            pltpu.VMEM((n, 8, lanes), jnp.float32),
            pltpu.SemaphoreType.DMA((6,)),
            pltpu.SemaphoreType.DMA((SLABS,)),
            pltpu.SemaphoreType.DMA((n,)),
            pltpu.SemaphoreType.DMA((n,)),
        ],
        compiler_params=pltpu.CompilerParams(collective_id=0, has_side_effects=True),
    )(turned)
    filtered = field.reshape(2, slab, HALF, lanes).transpose(0, 1, 3, 2).reshape(2, slab, width)
    return filtered, profile


def solution(mesh):
    return jax.shard_map(
        functools.partial(per_device, mesh.shape["rows"]),
        mesh=mesh,
        in_specs=(P(("groups", "rows"), None),),
        out_specs=(P(None, ("groups", "rows"), None), P("groups", None)),
        check_vma=False,
    )
```

```python
import functools
import math

import jax
import jax.numpy as jnp
from jax import lax
from jax.experimental import pallas as pl
from jax.experimental.pallas import tpu as pltpu
from jax.sharding import PartitionSpec as P

ITERS = 3
HALF = 16
WIN = 32
EPS = 1e-06
REACH = ITERS
SLABS = 2 * REACH + 1
PITCH = HALF + 1
AREA = HALF * HALF
SKEW = 8


def rotated(value, cosine, sine):
    real, imag = value
    if sine == 0.0:
        return value
    if cosine == 0.0:
        return (imag, -real) if sine > 0 else (-imag, real)
    if abs(cosine - sine) < 1e-12:
        return ((real + imag) * cosine, (imag - real) * cosine)
    if abs(cosine + sine) < 1e-12:
        return ((real - imag) * cosine, (imag + real) * cosine)
    return (real * cosine + imag * sine, imag * cosine - real * sine)


def twiddle(power, size):
    power = power % size
    exact = {0: (1.0, 0.0), size // 4: (0.0, 1.0), size // 2: (-1.0, 0.0), 3 * size // 4: (0.0, -1.0)}
    if power in exact:
        return exact[power]
    angle = 2.0 * math.pi * power / size
    return math.cos(angle), math.sin(angle)


def plus(a, b):
    return (a[0] + b[0], a[1] + b[1])


def minus(a, b):
    return (a[0] - b[0], a[1] - b[1])


def fft(values):
    size = len(values)
    if size == 1:
        return values
    if size == 2:
        return [plus(values[0], values[1]), minus(values[0], values[1])]
    even = fft(values[0::2])
    first = fft(values[1::4])
    third = fft(values[3::4])
    quarter = size // 4
    result = [None] * size
    for k in range(quarter):
        p = rotated(first[k], *twiddle(k, size))
        q = rotated(third[k], *twiddle(3 * k, size))
        total = plus(p, q)
        gap = minus(p, q)
        result[k] = plus(even[k], total)
        result[k + 2 * quarter] = minus(even[k], total)
        base = even[k + quarter]
        result[k + quarter] = (base[0] + gap[1], base[1] - gap[0])
        result[k + 3 * quarter] = (base[0] - gap[1], base[1] + gap[0])
    return result


def inverse_fft(values):
    swapped = fft([(imag, real) for real, imag in values])
    return [(real, imag) for imag, real in swapped]


def ramp(offset):
    return 1.0 - abs(offset - (WIN - 1) / 2) / HALF


SIN = [(-1.0) ** k / math.factorial(2 * k + 1) for k in range(7)]
COS = [(-1.0) ** k / math.factorial(2 * k) for k in range(8)]


def polynomial(coefficients, x):
    total = coefficients[-1]
    for c in coefficients[-2::-1]:
        total = total * x + c
    return total


def cos_sin(x):
    u = x * 0.5
    u2 = u * u
    s = u * polynomial(SIN, u2)
    c = polynomial(COS, u2)
    return 1.0 - 2.0 * s * s, 2.0 * s * c


def kernel(n, lanes, ph_ref, out_ref, prof_ref, ph, z, spec, cols, mine, heard,
           send_sem, recv_sem, tell_sem, hear_sem):
    me = lax.axis_index("rows")

    def inside(index):
        return jnp.logical_and(index >= 0, index < n)

    barrier = pltpu.get_barrier_semaphore()

    @pl.loop(1, n)
    def _(d):
        other = lax.rem(me + d, n)
        pl.semaphore_signal(barrier, inc=1, device_id={"rows": other}, device_id_type=pl.DeviceIdType.MESH)

    lane = lax.broadcasted_iota(jnp.int32, (8, lanes), 1)

    def next_block(x):
        return jnp.where(lane == lanes - 1, 0.0, pltpu.roll(x, lanes - 1, 1))

    def last_block(x):
        return jnp.where(lane == 0, 0.0, pltpu.roll(x, 1, 1))

    def enter(source, slot):
        @pl.loop(0, HALF)
        def _(t):
            for h in range(2):
                x = source[pl.ds(t * HALF + 8 * h, 8), :]
                c, s = cos_sin(x)
                z[0, slot, 0, pl.ds(t * HALF + 8 * h, 8), :] = c
                z[0, slot, 1, pl.ds(t * HALF + 8 * h, 8), :] = s

    def clear(buffer, slot):
        for c in range(2):
            z[buffer, slot, c, 0:AREA] = jnp.zeros((AREA, lanes), jnp.float32)

    enter(ph_ref, REACH)
    for slot in range(1, SLABS - 1):
        clear(1, slot)
    pl.semaphore_wait(barrier, n - 1)

    side = 1 - 2 * lax.rem(me, 2)

    def copy(source, d, target, index):
        slot = REACH + d - target
        return pltpu.make_async_remote_copy(
            src_ref=source,
            dst_ref=ph.at[slot],
            send_sem=send_sem.at[index],
            recv_sem=recv_sem.at[slot],
            device_id={"rows": me + target},
            device_id_type=pl.DeviceIdType.MESH,
        )

    direct = [(side, 0), (2 * side, 1), (-2 * side, 2), (-3 * side, 3)]
    relayed = [(2 * side, 4), (-2 * side, 5)]

    for target, index in direct:
        @pl.when(inside(me + target))
        def _(target=target, index=index):
            copy(ph_ref, 0, target, index).start()

    def landed(d):
        slot = REACH + d
        return pltpu.make_async_remote_copy(
            src_ref=ph_ref,
            dst_ref=ph.at[slot],
            send_sem=send_sem.at[0],
            recv_sem=recv_sem.at[slot],
            device_id={"rows": me + d},
            device_id_type=pl.DeviceIdType.MESH,
        )

    def relay():
        for d, index in relayed:
            @pl.when(inside(me + d))
            def _(d=d, index=index):
                landed(d).wait_recv()
                copy(ph.at[REACH + d], d, side, index).start()

    def arrive(d, waited):
        slot = REACH + d
        valid = inside(me + d)

        @pl.when(valid)
        def _():
            if not waited:
                landed(d).wait_recv()
            enter(ph.at[slot], slot)

        @pl.when(jnp.logical_not(valid))
        def _():
            clear(0, slot)

    def profile(buffer, step):
        def row(slot, t):
            real = z[buffer, slot, 0, pl.ds(t * HALF, HALF), :]
            imag = z[buffer, slot, 1, pl.ds(t * HALF, HALF), :]

            def after(x):
                first = next_block(x[0:8])[0:1]
                return jnp.concatenate([x[1:], first], axis=0)

            return real, imag, after(real), after(imag)

        def cross(ar, ai, br, bi):
            return ai * br - ar * bi

        def add(upper, lower, total):
            loop = (
                cross(upper[0], upper[1], upper[2], upper[3])
                + cross(upper[2], upper[3], lower[2], lower[3])
                + cross(lower[2], lower[3], lower[0], lower[1])
                + cross(lower[0], lower[1], upper[0], upper[1])
            )
            return total + loop * loop

        total = lax.fori_loop(
            0, HALF - 1,
            lambda t, total: add(row(REACH, t), row(REACH, t + 1), total),
            jnp.zeros((HALF, lanes), jnp.float32),
        )
        total = add(row(REACH, HALF - 1), row(REACH + 1, 0), total)
        mine[pl.ds(step, 1), :] = jnp.sum(total, axis=0, keepdims=True)

    def window_row(buffer, w):
        upper = REACH + w

        energy = jnp.zeros((8, lanes), jnp.float32)
        for h in range(2):
            values = []
            for t in range(WIN):
                at = pl.ds((t % HALF) * HALF + 8 * h, 8)
                values.append((z[buffer, upper + t // HALF, 0, at, :], z[buffer, upper + t // HALF, 1, at, :]))
            for real, imag in values:
                energy = energy + (real * real + imag * imag)
            for k, value in enumerate(fft(values)):
                for c in range(2):
                    spec[c, pl.ds(k * PITCH + 8 * h, 8), :] = value[c]
        energy = jnp.broadcast_to(jnp.sum(energy, axis=0, keepdims=True), (8, lanes))
        scale = 1.0 / (energy + next_block(energy) + EPS)

        @pl.loop(0, WIN // 8)
        def _(g):
            values = []
            for s in range(HALF):
                at = pl.ds(g * 8 * PITCH + s, 8, stride=PITCH)
                values.append((spec[0, at, :], spec[1, at, :]))
            values += [(next_block(real), next_block(imag)) for real, imag in values]
            shaped = []
            for real, imag in fft(values):
                ratio = jnp.maximum((real * real + imag * imag) * scale, 1e-37)
                gain = lax.rsqrt(lax.rsqrt(ratio))
                shaped.append((real * gain, imag * gain))
            back = inverse_fft(shaped)
            for s in range(HALF):
                near = ramp(s) / (WIN * WIN)
                far = ramp(s + HALF) / (WIN * WIN)
                for c in range(2):
                    joined = back[s][c] * near + last_block(back[s + HALF][c] * far)
                    cols[c, pl.ds(g * 8 * PITCH + s, 8, stride=PITCH), :] = joined

        for h in range(2):
            values = []
            for k in range(WIN):
                at = pl.ds(k * PITCH + 8 * h, 8)
                values.append((cols[0, at, :], cols[1, at, :]))
            for t, value in enumerate(inverse_fft(values)):
                at = pl.ds((t % HALF) * HALF + 8 * h, 8)
                for c in range(2):
                    z[1 - buffer, upper + t // HALF, c, at, :] += value[c] * ramp(t)

        @pl.when(me + w + 1 == n)
        def _():
            clear(1 - buffer, upper + 1)

    mine[...] = jnp.zeros_like(mine)

    def first_pass(slab, window, waited):
        arrive(slab * side, waited)
        w = window * side + (side - 1) // 2

        @pl.when(inside(me + w))
        def _():
            window_row(0, w)

    first_pass(1, 0, False)
    relay()
    first_pass(2, 1, True)

    @pl.loop(0, 2)
    def _(k):
        w = -1 - k
        slab = (-1 - k) * side

        @pl.when(k == 0)
        def _():
            arrive(slab, False)

        @pl.when(k == 1)
        def _():
            arrive(slab, True)

        below = w * side + (side - 1) // 2

        @pl.when(inside(me + below))
        def _():
            window_row(0, below)

    @pl.loop(0, 2)
    def _(k):
        slab = (3 - 6 * k) * side
        arrive(slab, False)
        below = (2 - 5 * k) * side + (side - 1) // 2

        @pl.when(inside(me + below))
        def _():
            window_row(0, below)

    profile(0, 0)

    def tell(d):
        other = lax.rem(me + d, n)
        return pltpu.make_async_remote_copy(
            src_ref=mine,
            dst_ref=heard.at[n - d],
            send_sem=tell_sem.at[d],
            recv_sem=hear_sem.at[n - d],
            device_id={"rows": other},
            device_id_type=pl.DeviceIdType.MESH,
        )

    for step in range(1, ITERS):
        buffer = step % 2
        reach = REACH - step
        profile(buffer, step)

        @pl.loop(REACH - reach, REACH + reach + 1)
        def _(slot):
            clear(1 - buffer, slot)

        if step == ITERS - 1:
            @pl.loop(1, n)
            def _(d):
                tell(d).start()

        @pl.loop(-reach, reach)
        def _(w):
            @pl.when(inside(me + w))
            def _():
                window_row(buffer, w)

    for c in range(2):
        out_ref[c] = z[ITERS % 2, REACH, c, 0:AREA]

    for target, index in direct:
        @pl.when(inside(me + target))
        def _(target=target, index=index):
            copy(ph_ref, 0, target, index).wait_send()

    for d, index in relayed:
        @pl.when(inside(me + d))
        def _(d=d, index=index):
            copy(ph.at[REACH + d], d, side, index).wait_send()

    def listen(d, total):
        tell(d).wait_send()
        pltpu.make_async_remote_copy(
            src_ref=mine,
            dst_ref=heard.at[d],
            send_sem=tell_sem.at[d],
            recv_sem=hear_sem.at[d],
            device_id={"rows": lax.rem(me + d, n)},
            device_id_type=pl.DeviceIdType.MESH,
        ).wait_recv()
        return total + heard[d]

    sums = lax.fori_loop(1, n, listen, mine[...])
    tiles = prof_ref.shape[1]
    per_tile = lanes // tiles
    rows = lax.broadcasted_iota(jnp.int32, (lanes, tiles), 0)
    low = lax.broadcasted_iota(jnp.int32, (lanes, tiles), 1) * per_tile
    member = jnp.where(jnp.logical_and(rows >= low, rows < low + per_tile), 1.0, 0.0)
    energy = jnp.dot(sums, member, precision=lax.Precision.HIGHEST, preferred_element_type=jnp.float32)
    prof_ref[...] = energy[:ITERS] / (HALF * n * 128.0)


def per_device(n, phase):
    slab, width = phase.shape
    assert slab == HALF and n % 2 == 0
    lanes = width // HALF
    turned = phase.reshape(slab, lanes, HALF).transpose(0, 2, 1).reshape(slab * HALF, lanes)
    field, profile = pl.pallas_call(
        functools.partial(kernel, n, lanes),
        out_shape=(
            jax.ShapeDtypeStruct((2, AREA, lanes), jnp.float32),
            jax.ShapeDtypeStruct((ITERS, width // 128), jnp.float32),
        ),
        in_specs=[pl.BlockSpec(memory_space=pltpu.VMEM)],
        out_specs=(pl.BlockSpec(memory_space=pltpu.VMEM), pl.BlockSpec(memory_space=pltpu.VMEM)),
        scratch_shapes=[
            pltpu.VMEM((SLABS, AREA, lanes), jnp.float32),
            pltpu.VMEM((2, SLABS, 2, AREA + SKEW, lanes), jnp.float32),
            pltpu.VMEM((2, WIN * PITCH + SKEW, lanes), jnp.float32),
            pltpu.VMEM((2, WIN * PITCH + SKEW, lanes), jnp.float32),
            pltpu.VMEM((8, lanes), jnp.float32),
            pltpu.VMEM((n, 8, lanes), jnp.float32),
            pltpu.SemaphoreType.DMA((6,)),
            pltpu.SemaphoreType.DMA((SLABS,)),
            pltpu.SemaphoreType.DMA((n,)),
            pltpu.SemaphoreType.DMA((n,)),
        ],
        compiler_params=pltpu.CompilerParams(collective_id=0, has_side_effects=True),
    )(turned)
    filtered = field.reshape(2, slab, HALF, lanes).transpose(0, 1, 3, 2).reshape(2, slab, width)
    return filtered, profile


def solution(mesh):
    return jax.shard_map(
        functools.partial(per_device, mesh.shape["rows"]),
        mesh=mesh,
        in_specs=(P(("groups", "rows"), None),),
        out_specs=(P(None, ("groups", "rows"), None), P("groups", None)),
        check_vma=False,
    )
```
